128 devices in a mesh: seq: 64 (over z, x, y), feat: 2 (over core).
Axes of the slice: x: 4, y: 4, z: 4, core: 2. Of those that a mesh axis runs over, the one named last changes fastest.
Arguments:
- tokens: bfloat16 [524288, 1280], P(('seq', 'feat')), may hold values from -12 to 12
- shot_starts: int32 [128], replicated, may hold values from 0 to 521728, as said below
- seed_offsets: int32 [128, 64], replicated, may hold values from 0 to 1023, as said below
- norm_gain: float32 [1280], replicated, may hold values from 0.5 to 1.5
- proj_weight: bfloat16 [1280, 8192], P(None, 'feat'), may hold values from -0.15625 to 0.15625
Outputs:
- projected: bfloat16 [8192, 8192], P('seq', 'feat')
The draws below stay inside these ranges and needn't reach their ends.
Inputs may be any that keep to these rules, and one draw needn't show every extreme that they name: shot_starts[0] = 0, the starts rise, and shot s starts within 1536 tokens of s * 4096, so a shot has 1024 to 7168 tokens. `seed_offsets`: each row holds 64 different offsets, all below 1024.
All inputs are finite; a program needn't handle non-finite values.
Results may differ from the reference program's by a relative error of at most 0.0055.
Values may be sent and summed in bfloat16 or wider, within the bound.
A program may use at most 128 MiB of HBM per device.

```python
import math
import jax
import jax.numpy as jnp
from jax import lax

D = 1280
P_SIZE = 8192
K = 64
ITERS = 3
TOK_DEV = 4096
HALF = 1536
MINLEN = 1024
LMAX = 7168
SHOTS = 128
TOKENS = 524288


def shot_layout(key):
    folded = jax.random.fold_in(key, 17)
    key_offset, key_pick, key_seed = jax.random.split(folded, 3)
    offsets = jax.random.randint(key_offset, (SHOTS,), -HALF, HALF + 1)
    chosen = jax.random.randint(key_pick, (), 1, SHOTS - 2)
    shot_index = jnp.arange(SHOTS)
    offsets = jnp.where(shot_index == chosen, HALF, offsets)
    offsets = jnp.where(shot_index == chosen + 1, -HALF, offsets)
    offsets = jnp.where(shot_index == chosen + 2, HALF, offsets)
    offsets = jnp.where(shot_index == 0, 0, offsets)
    shot_starts = (shot_index * TOK_DEV + offsets).astype(jnp.int32)
    seed_keys = jax.random.split(key_seed, SHOTS)
    seed_offsets = jax.vmap(lambda subkey: jax.random.permutation(subkey, MINLEN)[:K])(seed_keys)
    return (shot_starts, seed_offsets.astype(jnp.int32))


def draw_shot_starts(key, part):
    return shot_layout(key)[0]


def draw_seed_offsets(key, part):
    return shot_layout(key)[1]


def draw_tokens(key, part):
    shot_starts, seed_offsets = shot_layout(key)
    key_center, key_count, key_member, key_value = jax.random.split(jax.random.fold_in(key, 29), 4)
    position = jnp.arange(TOKENS, dtype=jnp.int32)
    shot_of = (jnp.searchsorted(shot_starts, position, side='right') - 1).astype(jnp.int32)
    cluster_counts = jax.random.randint(key_count, (SHOTS,), K // 2, 2 * K + 1)
    member_raw = jax.random.randint(key_member, (TOKENS,), 0, 1 << 20)
    member = member_raw % jnp.take(cluster_counts, shot_of)
    cluster_id = (shot_of * (2 * K) + member).astype(jnp.int32)
    centres = 0.6 * jnp.clip(jax.random.normal(key_center, (SHOTS * 2 * K, D), jnp.float32), -4.0, 4.0)
    noise = 0.5 * jnp.clip(jax.random.normal(key_value, (TOKENS, D), jnp.float32), -4.0, 4.0)
    values = jnp.take(centres, cluster_id, axis=0) + noise
    return jnp.clip(values, -12.0, 12.0).astype(jnp.bfloat16)


def level_of(stream_key, dims, cuts, smallest, high):
    loudness = 1.0
    for axis_at, shards_of in cuts:
        draws = jax.random.uniform(jax.random.fold_in(jax.random.fold_in(stream_key, 6), axis_at), (shards_of,), jnp.float32, smallest / len(cuts), high / len(cuts))
        loudness = loudness * jnp.repeat(jnp.exp(draws), dims[axis_at] // shards_of).reshape((-1,) + (1,) * (len(dims) - 1 - axis_at))
    return loudness


def bell_draw(stream_key, dims, width, limit, pieces=(), held_as=jnp.bfloat16):
    loudness = level_of(stream_key, dims, pieces, -0.22, 0.18) if pieces else 1.0
    array = jax.random.normal(stream_key, dims, jnp.float32) * width * loudness
    return jnp.minimum(jnp.maximum(array, -limit), limit).astype(held_as)


def setup_inputs(seed: int = 0) -> dict:
    keys = jax.random.split(jax.random.key(seed), 6)
    tokens = draw_tokens(jax.random.fold_in(keys[5], 71), 0)
    shot_starts = draw_shot_starts(jax.random.fold_in(keys[5], 71), 0)
    seed_offsets = draw_seed_offsets(jax.random.fold_in(keys[5], 71), 0)
    norm_gain = jnp.clip(1.0 + 0.1 * jax.random.normal(keys[3], (D,), jnp.float32), 0.5, 1.5)
    proj_weight = bell_draw(keys[4], (D, P_SIZE), D ** -0.5, 0.15625, ((1, 2),))
    return dict(tokens=tokens, shot_starts=shot_starts, seed_offsets=seed_offsets, norm_gain=norm_gain, proj_weight=proj_weight)


def shot_centroids(tokens, norm_gain, shot_begin, shot_finish, seed_row):
    token_total = tokens.shape[0]
    window_start = jnp.minimum(shot_begin, token_total - LMAX).astype(jnp.int32)
    window = lax.dynamic_slice_in_dim(tokens, window_start, LMAX, 0)
    position = window_start + jnp.arange(LMAX, dtype=jnp.int32)
    inside = (position >= shot_begin) & (position < shot_finish)
    seed_rows = (shot_begin + seed_row).astype(jnp.int32)
    centroid = jnp.take(tokens, seed_rows, axis=0).astype(jnp.float32)
    factor = 1.0 / math.sqrt(D)
    for iteration in range(ITERS):
        scores = jnp.dot(window, centroid.astype(jnp.bfloat16).T, preferred_element_type=jnp.float32) * factor
        weights = jax.nn.softmax(scores, axis=-1)
        weights = jnp.where(inside[:, None], weights, jnp.zeros_like(weights))
        shot_mass = lax.optimization_barrier(jnp.sum(weights, axis=0))
        shot_sums = lax.dot_general(weights.astype(jnp.bfloat16), window, (((0,), (0,)), ((), ())), preferred_element_type=jnp.float32)
        centroid = shot_sums / shot_mass[:, None]
    spread = jnp.sqrt(lax.optimization_barrier(jnp.mean(centroid * centroid, axis=-1, keepdims=True)) + 1e-06)
    return (centroid / spread * norm_gain).astype(jnp.bfloat16)

def reference(tokens, shot_starts, seed_offsets, norm_gain, proj_weight):
    token_total = tokens.shape[0]
    shot_ends = jnp.concatenate([shot_starts[1:], jnp.full((1,), token_total, jnp.int32)])
    normed = lax.map(lambda shot_item: shot_centroids(tokens, norm_gain, shot_item[0], shot_item[1], shot_item[2]), (shot_starts, shot_ends, seed_offsets))
    flat_rows = normed.reshape(SHOTS * K, D)
    return jnp.dot(flat_rows, proj_weight, preferred_element_type=jnp.float32).astype(jnp.bfloat16)
```

```python
import functools
import math

import jax
import jax.numpy as jnp
from jax import lax
from jax.experimental import pallas as pl
from jax.experimental.pallas import tpu as pltpu
from jax.sharding import PartitionSpec as P

MESH = pl.DeviceIdType.MESH
ITERS = 3
ROUNDS = ITERS + 1
K = 64
CHUNK = 256
TILE = 256
COLS = 512


def kernel(
    seq_size,
    starts,
    seeds,
    gain,
    tok_hbm,
    w_hbm,
    out_hbm,
    x,
    wp,
    outs,
    s,
    wt,
    c,
    po,
    px,
    pnb,
    si,
    qo,
    tb,
    ub,
    co,
    ci,
    mn,
    mo,
    mi,
    mq,
    mt,
    mu,
    rec,
    cent,
    ns,
    nm,
    x_sem,
    w_sem,
    o_sem,
    p_send,
    p_recv,
    t_send,
    t_recv,
    c_send,
    c_recv,
    mp_send,
    mp_recv,
    mt_send,
    mt_recv,
    n_send,
    n_recv,
):
    chunks, rows, _ = x.shape
    half = rows // 2
    tiles = half // TILE
    col_tiles = wp.shape[0]
    width = chunks * CHUNK
    f32, bf16 = jnp.float32, jnp.bfloat16

    seq = lax.axis_index("seq")
    feat = lax.axis_index("feat")
    me = seq * 2 + feat
    count = seq_size * 2
    inner = (seq, 1 - feat)
    outer_seq = seq + 2 * feat - 1
    has_outer = jnp.logical_and(outer_seq >= 0, outer_seq < seq_size)
    outer = (outer_seq, 1 - feat)
    h_in, h_out = 1 - feat, feat

    def token_copy(f):
        return pltpu.make_async_copy(
            tok_hbm.at[:, pl.ds(pl.multiple_of(f * CHUNK, CHUNK), CHUNK)], x.at[f], x_sem.at[f]
        )

    def weight_copy(n):
        return pltpu.make_async_copy(
            w_hbm.at[:, pl.ds(pl.multiple_of(n * COLS, COLS), COLS)], wp.at[n], w_sem.at[n]
        )

    def out_copy(n):
        return pltpu.make_async_copy(
            outs.at[n], out_hbm.at[:, pl.ds(pl.multiple_of(n * COLS, COLS), COLS)], o_sem.at[n]
        )

    def remote(src, dst, send, recv, device):
        return pltpu.make_async_remote_copy(
            src_ref=src,
            dst_ref=dst,
            send_sem=send,
            recv_sem=recv,
            device_id=device,
            device_id_type=MESH,
        )

    def p_copy(r, f):
        return remote(si.at[r, f], qo.at[r, f], p_send.at[r, f], p_recv.at[r, f], inner)

    def t_copy(r, f):
        return remote(tb.at[r, f], ub.at[r, f], t_send.at[r, f], t_recv.at[r, f], outer)

    def c_copy(r, f):
        return remote(co.at[r, f], ci.at[r, f], c_send.at[r, f], c_recv.at[r, f], inner)

    def mp_copy(r):
        return remote(mi.at[r], mq.at[r], mp_send.at[r], mp_recv.at[r], inner)

    def mt_copy(r):
        return remote(mt.at[r], mu.at[r], mt_send.at[r], mt_recv.at[r], outer)

    def n_copy():
        return remote(ns, nm.at[pl.ds(feat * K, K)], n_send, n_recv, inner)

    @pl.loop(0, chunks)
    def _(f):
        token_copy(f).start()

    barrier = pltpu.get_barrier_semaphore()
    pl.semaphore_signal(barrier, inc=1, device_id=inner, device_id_type=MESH)

    @pl.when(has_outer)
    def _():
        pl.semaphore_signal(barrier, inc=1, device_id=outer, device_id_type=MESH)

    base = me * rows
    start = starts[me] - base
    following = starts[jnp.minimum(me + 1, count - 1)]
    end = jnp.where(me == count - 1, count * rows, following) - base

    def is_mine(shape):
        first = jnp.full(shape, start, jnp.int32) < 0
        last = jnp.full(shape, end, jnp.int32) >= rows
        left = jnp.full(shape, feat, jnp.int32) == 0
        return jnp.logical_or(
            jnp.logical_and(left, first), jnp.logical_and(jnp.logical_not(left), last)
        )

    @pl.when(jnp.logical_not(has_outer))
    def _():
        ub[...] = jnp.zeros_like(ub)
        mu[...] = jnp.zeros_like(mu)

    def column(row, offset):
        spread = jnp.broadcast_to(seeds[pl.ds(row, 1), :].astype(f32), (K, K))
        return spread.T[:, :1].astype(jnp.int32) + offset

    own_at = column(me, start)
    next_at = column(jnp.minimum(me + 1, count - 1), end)

    def lanes(h, t):
        return lax.broadcasted_iota(jnp.int32, (K, TILE), 1) + (h * half + t * TILE)

    def place(t):
        return pl.ds(pl.multiple_of(t * TILE, TILE), TILE)

    def fold(w):
        total = w[:, :128]
        for i in range(1, TILE // 128):
            total = total + w[:, i * 128 : (i + 1) * 128]
        return total

    def put(h, t, nb, own):
        wt[h, :K, place(t)] = nb.astype(bf16)
        wt[h, K:, place(t)] = own.astype(bf16)

    zero = jnp.zeros((K, 128), f32)

    def note_mass(r, nbs, own):
        def total(m):
            return jnp.broadcast_to(jnp.sum(m, axis=1, keepdims=True), (K, 128))

        mn[0] = total(nbs[0])
        mn[1] = total(nbs[1])
        mo[...] = total(own)
        mi[r] = mn[h_in]
        mp_copy(r).start()

    nbs, own_mass = [], zero
    for h in range(2):

        def seed_tile(t, carry, h=h):
            nb_mass, own_mass = carry
            at = lanes(h, t)
            own = (at == own_at).astype(f32)
            nb = (at == next_at).astype(f32) if h else jnp.zeros((K, TILE), f32)
            put(h, t, nb, own)
            return nb_mass + fold(nb), own_mass + fold(own)

        nb_mass, own_mass = lax.fori_loop(0, tiles, seed_tile, (zero, own_mass))
        nbs.append(nb_mass)

    pl.semaphore_wait(barrier, 1 + has_outer.astype(jnp.int32))

    note_mass(0, nbs, own_mass)

    def wide(m):
        return jnp.concatenate([m] * (CHUNK // 128), axis=1)

    def round_body(r, carry):
        def sums(f):
            @pl.when(r == 0)
            def _():
                token_copy(f).wait()

            low = jnp.dot(wt[0], x[f, :half], preferred_element_type=f32)
            high = jnp.dot(wt[1], x[f, half:], preferred_element_type=f32)
            pnb[0] = low[:K]
            pnb[1] = high[:K]
            po[f] = low[K:] + high[K:]
            px[f] = pnb[h_out]
            si[r, f] = pnb[h_in]
            p_copy(r, f).start()

        def pass_on(f):
            p_copy(r, f).wait_recv()
            chip = po[f] + qo[r, f]
            po[f] = chip
            tb[r, f] = jnp.where(is_mine((K, CHUNK)), chip, px[f]).astype(bf16)

            @pl.when(has_outer)
            def _():
                t_copy(r, f).start()

        def pass_mass_on():
            mp_copy(r).wait_recv()
            chip = mo[...] + mq[r]
            mo[...] = chip
            mt[r] = jnp.where(is_mine((K, 128)), chip, mn[h_out])

            @pl.when(has_outer)
            def _():
                mt_copy(r).start()

        @pl.loop(0, chunks + 2)
        def _(f):
            @pl.when(f < chunks)
            def _():
                sums(f)

            @pl.when(f == 2)
            def _():
                pass_mass_on()

            @pl.when(f >= 2)
            def _():
                pass_on(f - 2)

        @pl.when(r == 0)
        def _():
            @pl.loop(0, col_tiles)
            def _(n):
                weight_copy(n).start()

        s[...] = jnp.zeros_like(s)

        @pl.when(has_outer)
        def _():
            mt_copy(r).wait_recv()

        mine = is_mine((K, 128))
        m_own = mo[...] + jnp.where(mine, mu[r], 0.0)
        m_nb = mn[h_out] + jnp.where(mine, 0.0, mu[r])
        rec[0] = 1.0 / m_own
        rec[1] = 1.0 / jnp.where(m_nb > 0.0, m_nb, 1.0)

        def arrive(f):
            @pl.when(has_outer)
            def _():
                t_copy(r, f).wait_recv()

            mine = is_mine((K, CHUNK))
            u = ub[r, f].astype(f32)
            own = (po[f] + jnp.where(mine, u, 0.0)) * wide(rec[0])
            cent[f] = own
            return (px[f] + jnp.where(mine, 0.0, u)) * wide(rec[1])

        def spread(f):
            nb = arrive(f)
            own = cent[f].astype(bf16)
            co[r, f] = own
            c_copy(r, f).start()
            c[0, f, K:] = own
            c[1, f, K:] = own
            c[h_out, f, :K] = nb.astype(bf16)

        def score(f):
            c_copy(r, f).wait_recv()
            c[h_in, f, :K] = ci[r, f]
            for h in range(2):
                s[h * half : (h + 1) * half] += lax.dot_general(
                    x[f, h * half : (h + 1) * half],
                    c[h, f],
                    (((1,), (1,)), ((), ())),
                    preferred_element_type=f32,
                )

        def soften():
            scale = math.log2(math.e) / math.sqrt(width)
            nbs, own_mass = [], zero
            for h in range(2):

                def tile(t, carry, h=h):
                    nb_mass, own_mass = carry
                    at = pl.ds(pl.multiple_of(h * half + t * TILE, TILE), TILE)
                    flat = s[at].T
                    where = lanes(h, t)
                    is_nb = (where >= end) if h else (where < start)
                    mixed = jnp.where(is_nb, flat[:K], flat[K:])
                    e = jnp.exp2((mixed - jnp.max(mixed, axis=0, keepdims=True)) * scale)
                    w = e * (1.0 / jnp.sum(e, axis=0, keepdims=True))
                    nb = jnp.where(is_nb, w, 0.0)
                    own = jnp.where(is_nb, 0.0, w)
                    put(h, t, nb, own)
                    return nb_mass + fold(nb), own_mass + fold(own)

                nb_mass, own_mass = lax.fori_loop(0, tiles, tile, (zero, own_mass))
                nbs.append(nb_mass)
            note_mass(r + 1, nbs, own_mass)

        @pl.when(r < ITERS)
        def _():
            @pl.loop(0, chunks + 2)
            def _(f):
                @pl.when(f < chunks)
                def _():
                    spread(f)

                @pl.when(f >= 2)
                def _():
                    score(f - 2)

            soften()

        @pl.when(r == ITERS)
        def _():
            @pl.loop(0, chunks)
            def _(f):
                arrive(f)

        return carry

    lax.fori_loop(0, ROUNDS, round_body, 0)

    square = jnp.zeros((K, 1), f32)
    for f in range(chunks):
        square = square + jnp.sum(cent[f] * cent[f], axis=1, keepdims=True)
    inverse = 1.0 / jnp.sqrt(square / width + 1e-06)
    for f in range(chunks):
        at = slice(f * CHUNK, (f + 1) * CHUNK)
        normed = (cent[f] * inverse * gain[:, at]).astype(bf16)
        ns[:, at] = normed
        nm[pl.ds(pl.multiple_of(feat * K, K), K), at] = normed
    n_copy().start()
    n_copy().wait_recv()

    @pl.loop(0, col_tiles)
    def _(n):
        weight_copy(n).wait()
        outs[n] = jnp.dot(nm[...], wp[n], preferred_element_type=f32).astype(bf16)
        out_copy(n).start()

    n_copy().wait_send()

    @pl.loop(0, ROUNDS)
    def _(r):
        mp_copy(r).wait_send()

        @pl.when(has_outer)
        def _():
            mt_copy(r).wait_send()

        @pl.loop(0, chunks)
        def _(f):
            p_copy(r, f).wait_send()

            @pl.when(r < ITERS)
            def _():
                c_copy(r, f).wait_send()

            @pl.when(has_outer)
            def _():
                t_copy(r, f).wait_send()

    @pl.loop(0, col_tiles)
    def _(n):
        out_copy(n).wait()


def on_device(seq_size, tokens, shot_starts, seed_offsets, norm_gain, proj_weight):
    rows, width = tokens.shape
    columns = proj_weight.shape[1]
    chunks = width // CHUNK
    col_tiles = columns // COLS
    half = rows // 2
    f32, bf16 = jnp.float32, jnp.bfloat16
    vmem, dma = pltpu.VMEM, pltpu.SemaphoreType.DMA
    piece = (K, CHUNK)
    return pl.pallas_call(
        functools.partial(kernel, seq_size),
        out_shape=jax.ShapeDtypeStruct((2 * K, columns), bf16),
        in_specs=[
            pl.BlockSpec(memory_space=pltpu.SMEM),
            pl.BlockSpec(memory_space=pltpu.VMEM),
            pl.BlockSpec(memory_space=pltpu.VMEM),
            pl.BlockSpec(memory_space=pl.ANY),
            pl.BlockSpec(memory_space=pl.ANY),
        ],
        out_specs=pl.BlockSpec(memory_space=pl.ANY),
        scratch_shapes=[
            vmem((chunks, rows, CHUNK), bf16),
            vmem((col_tiles, width, COLS), bf16),
            vmem((col_tiles, 2 * K, COLS), bf16),
            vmem((rows, 2 * K), f32),
            vmem((2, 2 * K, half), bf16),
            vmem((2, chunks, 2 * K, CHUNK), bf16),
            vmem((chunks, *piece), f32),
            vmem((chunks, *piece), f32),
            vmem((2, *piece), f32),
            vmem((ROUNDS, chunks, *piece), f32),
            vmem((ROUNDS, chunks, *piece), f32),
            vmem((ROUNDS, chunks, *piece), bf16),
            vmem((ROUNDS, chunks, *piece), bf16),
            vmem((ITERS, chunks, *piece), bf16),
            vmem((ITERS, chunks, *piece), bf16),
            vmem((2, K, 128), f32),
            vmem((K, 128), f32),
            vmem((ROUNDS, K, 128), f32),
            vmem((ROUNDS, K, 128), f32),
            vmem((ROUNDS, K, 128), f32),
            vmem((ROUNDS, K, 128), f32),
            vmem((2, K, 128), f32),
            vmem((chunks, *piece), f32),
            vmem((K, width), bf16),
            vmem((2 * K, width), bf16),
            dma((chunks,)),
            dma((col_tiles,)),
            dma((col_tiles,)),
            dma((ROUNDS, chunks)),
            dma((ROUNDS, chunks)),
            dma((ROUNDS, chunks)),
            dma((ROUNDS, chunks)),
            dma((ITERS, chunks)),
            dma((ITERS, chunks)),
            dma((ROUNDS,)),
            dma((ROUNDS,)),
            dma((ROUNDS,)),
            dma((ROUNDS,)),
            dma,
            dma,
        ],
        compiler_params=pltpu.CompilerParams(
            collective_id=0, has_side_effects=True, vmem_limit_bytes=60 * 2**20
        ),
    )(shot_starts, seed_offsets, norm_gain[None, :], tokens, proj_weight)


def solution(mesh):
    in_specs = (P(("seq", "feat"), None), P(), P(), P(), P(None, "feat"))
    out_specs = P("seq", "feat")
    return jax.shard_map(
        functools.partial(on_device, mesh.shape["seq"]),
        mesh=mesh,
        in_specs=in_specs,
        out_specs=out_specs,
        check_vma=False,
    )
```

```python
import functools
import math

import jax
import jax.numpy as jnp
from jax import lax
from jax.experimental import pallas as pl
from jax.experimental.pallas import tpu as pltpu
from jax.sharding import PartitionSpec as P

MESH = pl.DeviceIdType.MESH
ITERS = 3
ROUNDS = ITERS + 1
K = 64
CHUNK = 256
TILE = 256
COLS = 512
LAG = 3


def kernel(
    seq_size,
    starts,
    seeds,
    gain,
    tok_hbm,
    w_hbm,
    out_hbm,
    x,
    xt,
    wp,
    outs,
    st,
    wt,
    c,
    po,
    px,
    si,
    qo,
    tb,
    ub,
    co,
    ci,
    mf,
    mx,
    mo,
    mi,
    mq,
    mt,
    mu,
    rec,
    cent,
    ns,
    nm,
    x_sem,
    w_sem,
    o_sem,
    p_send,
    p_recv,
    t_send,
    t_recv,
    c_send,
    c_recv,
    mp_send,
    mp_recv,
    mt_send,
    mt_recv,
    n_send,
    n_recv,
):
    chunks, _, half, _ = x.shape
    rows = 2 * half
    tiles = half // TILE
    col_tiles = wp.shape[0]
    width = chunks * CHUNK
    f32, bf16 = jnp.float32, jnp.bfloat16

    seq = lax.axis_index("seq")
    feat = lax.axis_index("feat")
    me = seq * 2 + feat
    count = seq_size * 2
    inner = (seq, 1 - feat)
    outer_seq = seq + 2 * feat - 1
    has_outer = jnp.logical_and(outer_seq >= 0, outer_seq < seq_size)
    outer = (outer_seq, 1 - feat)
    h_in, h_out = 1 - feat, feat

    def token_copy(f, h):
        return pltpu.make_async_copy(
            tok_hbm.at[
                pl.ds(pl.multiple_of(h * half, half), half),
                pl.ds(pl.multiple_of(f * CHUNK, CHUNK), CHUNK),
            ],
            x.at[f, h],
            x_sem.at[f, h],
        )

    def weight_copy(n):
        return pltpu.make_async_copy(
            w_hbm.at[:, pl.ds(pl.multiple_of(n * COLS, COLS), COLS)], wp.at[n], w_sem.at[n]
        )

    def out_copy(n):
        return pltpu.make_async_copy(
            outs.at[n], out_hbm.at[:, pl.ds(pl.multiple_of(n * COLS, COLS), COLS)], o_sem.at[n]
        )

    def remote(src, dst, send, recv, device):
        return pltpu.make_async_remote_copy(
            src_ref=src,
            dst_ref=dst,
            send_sem=send,
            recv_sem=recv,
            device_id=device,
            device_id_type=MESH,
        )

    def p_copy(r, f):
        return remote(si.at[r, f], qo.at[r, f], p_send.at[r, f], p_recv.at[r, f], inner)

    def t_copy(r, f):
        return remote(tb.at[r, f], ub.at[r, f], t_send.at[r, f], t_recv.at[r, f], outer)

    def c_copy(r, f):
        return remote(co.at[r, f], ci.at[r, f], c_send.at[r, f], c_recv.at[r, f], inner)

    def mp_copy(r):
        return remote(mi.at[r], mq.at[r], mp_send.at[r], mp_recv.at[r], inner)

    def mt_copy(r):
        return remote(mt.at[r], mu.at[r], mt_send.at[r], mt_recv.at[r], outer)

    def n_copy():
        return remote(ns, nm.at[pl.ds(feat * K, K)], n_send, n_recv, inner)

    @pl.loop(0, chunks)
    def _(f):
        token_copy(f, h_in).start()

    @pl.loop(0, chunks)
    def _(f):
        token_copy(f, h_out).start()

    barrier = pltpu.get_barrier_semaphore()
    pl.semaphore_signal(barrier, inc=1, device_id=inner, device_id_type=MESH)

    @pl.when(has_outer)
    def _():
        pl.semaphore_signal(barrier, inc=1, device_id=outer, device_id_type=MESH)

    base = me * rows
    start = starts[me] - base
    after = jnp.minimum(me + 1, count - 1)
    end = jnp.where(me == count - 1, count * rows, starts[after]) - base

    def is_mine(shape):
        first = jnp.full(shape, start, jnp.int32) < 0
        last = jnp.full(shape, end, jnp.int32) >= rows
        left = jnp.full(shape, feat, jnp.int32) == 0
        return jnp.logical_or(
            jnp.logical_and(left, first), jnp.logical_and(jnp.logical_not(left), last)
        )

    @pl.when(jnp.logical_not(has_outer))
    def _():
        ub[...] = jnp.zeros_like(ub)
        mu[...] = jnp.zeros_like(mu)

    def column(shot, offset):
        shots = lax.broadcasted_iota(jnp.int32, seeds.shape, 1)
        picked = jnp.where(shots == shot, seeds[...], 0).astype(f32)
        return jnp.sum(picked, axis=1, keepdims=True).astype(jnp.int32) + offset

    own_at = column(me, start)
    next_at = column(after, end)

    def place(t):
        return pl.ds(pl.multiple_of(t * TILE, TILE), TILE)

    def fold(w):
        total = w[:, :128]
        for i in range(1, TILE // 128):
            total = total + w[:, i * 128 : (i + 1) * 128]
        return total

    def put(h, t, nb, own):
        wt[h, :K, place(t)] = nb.astype(bf16)
        wt[h, K:, place(t)] = own.astype(bf16)

    zero = jnp.zeros((K, 128), f32)

    def seed_weights(h):
        def tile(t, carry):
            nb_mass, own_mass = carry
            at = lax.broadcasted_iota(jnp.int32, (K, TILE), 1) + (h * half + t * TILE)
            own = (at == own_at).astype(f32)
            nb = (at == next_at).astype(f32)
            put(h, t, nb, own)
            return nb_mass + fold(nb), own_mass + fold(own)

        mf[h, 0], mf[h, 1] = lax.fori_loop(0, tiles, tile, (zero, zero))

    def soften(h):
        scale = math.log2(math.e) / math.sqrt(width)

        def tile(t, carry):
            nb_mass, own_mass = carry
            at = lax.broadcasted_iota(jnp.int32, (1, TILE), 1) + (h * half + t * TILE)
            is_nb = jnp.logical_or(at < start, at >= end)
            mixed = jnp.where(is_nb, st[h, :K, place(t)], st[h, K:, place(t)])
            e = jnp.exp2((mixed - jnp.max(mixed, axis=0, keepdims=True)) * scale)
            w = e * (1.0 / jnp.sum(e, axis=0, keepdims=True))
            nb = jnp.where(is_nb, w, 0.0)
            own = jnp.where(is_nb, 0.0, w)
            put(h, t, nb, own)
            return nb_mass + fold(nb), own_mass + fold(own)

        mf[h, 0], mf[h, 1] = lax.fori_loop(0, tiles, tile, (zero, zero), unroll=2)

    seed_weights(h_in)
    seed_weights(h_out)

    pl.semaphore_wait(barrier, 1 + has_outer.astype(jnp.int32))

    def wide(m):
        return jnp.concatenate([m] * (CHUNK // 128), axis=1)

    def round_body(r, carry):
        def send_mass():
            def total(m):
                return jnp.broadcast_to(jnp.sum(m, axis=1, keepdims=True), (K, 128))

            mi[r] = total(mf[h_in, 0])
            mp_copy(r).start()
            mx[...] = total(mf[h_out, 0])
            mo[...] = total(mf[0, 1] + mf[1, 1])

        def pass_mass_on():
            mp_copy(r).wait_recv()
            chip = mo[...] + mq[r]
            mo[...] = chip
            mt[r] = jnp.where(is_mine((K, 128)), chip, mx[...])

            @pl.when(has_outer)
            def _():
                mt_copy(r).start()

        def partial(f, h):
            @pl.when(r == 0)
            def _():
                token_copy(f, h).wait()

            return jnp.dot(wt[h], x[f, h], preferred_element_type=f32)

        def pass_on(f):
            p_copy(r, f).wait_recv()
            chip = po[f] + qo[r, f]
            po[f] = chip
            tb[r, f] = jnp.where(is_mine((K, CHUNK)), chip, px[f]).astype(bf16)

            @pl.when(has_outer)
            def _():
                t_copy(r, f).start()

        @pl.loop(0, chunks)
        def _(f):
            sums = partial(f, h_in)
            si[r, f] = sums[:K]
            p_copy(r, f).start()
            po[f] = sums[K:]

            @pl.when(f == 0)
            def _():
                send_mass()

        @pl.loop(0, chunks + 1)
        def _(f):
            @pl.when(f < chunks)
            def _():
                sums = partial(f, h_out)
                px[f] = sums[:K]
                po[f] += sums[K:]

            @pl.when(f == 1)
            def _():
                pass_mass_on()

            @pl.when(f >= 1)
            def _():
                pass_on(f - 1)

        @pl.when(r == 0)
        def _():
            @pl.loop(0, col_tiles)
            def _(n):
                weight_copy(n).start()

            @pl.loop(0, chunks)
            def _(f):
                for h in range(2):
                    for t in range(tiles):
                        at = slice(t * TILE, (t + 1) * TILE)
                        xt[f, h, :, at] = x[f, h, at].T

        st[...] = jnp.zeros_like(st)

        @pl.when(has_outer)
        def _():
            mt_copy(r).wait_recv()

        mine = is_mine((K, 128))
        m_own = mo[...] + jnp.where(mine, mu[r], 0.0)
        m_nb = mx[...] + jnp.where(mine, 0.0, mu[r])
        rec[0] = 1.0 / m_own
        rec[1] = 1.0 / jnp.where(m_nb > 0.0, m_nb, 1.0)

        def arrive(f):
            @pl.when(has_outer)
            def _():
                t_copy(r, f).wait_recv()

            mine = is_mine((K, CHUNK))
            u = ub[r, f].astype(f32)
            own = (po[f] + jnp.where(mine, u, 0.0)) * wide(rec[0])
            cent[f] = own
            return own, (px[f] + jnp.where(mine, 0.0, u)) * wide(rec[1])

        def spread(f):
            own, nb = arrive(f)
            own = own.astype(bf16)
            co[r, f] = own
            c_copy(r, f).start()
            c[0, f, K:] = own
            c[1, f, K:] = own
            c[h_out, f, :K] = nb.astype(bf16)

        def score(f, h):
            for t in range(half // COLS):
                at = slice(t * COLS, (t + 1) * COLS)
                st[h, :, at] += jnp.dot(c[h, f], xt[f, h, :, at], preferred_element_type=f32)

        def score_inner(f):
            c_copy(r, f).wait_recv()
            c[h_in, f, :K] = ci[r, f]
            score(f, h_in)

        @pl.when(r < ITERS)
        def _():
            @pl.loop(0, chunks)
            def _(f):
                spread(f)
                score(f, h_out)

                @pl.when(f >= LAG)
                def _():
                    score_inner(f - LAG)

            soften(h_out)

            @pl.loop(chunks - LAG, chunks)
            def _(f):
                score_inner(f)

            soften(h_in)

        @pl.when(r == ITERS)
        def _():
            @pl.loop(0, chunks)
            def _(f):
                arrive(f)

        return carry

    lax.fori_loop(0, ROUNDS, round_body, 0)

    square = jnp.zeros((K, 1), f32)
    for f in range(chunks):
        square = square + jnp.sum(cent[f] * cent[f], axis=1, keepdims=True)
    inverse = 1.0 / jnp.sqrt(square / width + 1e-06)
    for f in range(chunks):
        at = slice(f * CHUNK, (f + 1) * CHUNK)
        normed = (cent[f] * inverse * gain[at][None, :]).astype(bf16)
        ns[:, at] = normed
        nm[pl.ds(pl.multiple_of(feat * K, K), K), at] = normed
    n_copy().start()
    n_copy().wait_recv()

    @pl.loop(0, col_tiles)
    def _(n):
        weight_copy(n).wait()
        outs[n] = jnp.dot(nm[...], wp[n], preferred_element_type=f32).astype(bf16)
        out_copy(n).start()

    n_copy().wait_send()

    @pl.loop(0, ROUNDS)
    def _(r):
        mp_copy(r).wait_send()

        @pl.when(has_outer)
        def _():
            mt_copy(r).wait_send()

        @pl.loop(0, chunks)
        def _(f):
            p_copy(r, f).wait_send()

            @pl.when(r < ITERS)
            def _():
                c_copy(r, f).wait_send()

            @pl.when(has_outer)
            def _():
                t_copy(r, f).wait_send()

    @pl.loop(0, col_tiles)
    def _(n):
        out_copy(n).wait()


def on_device(seq_size, tokens, shot_starts, seed_offsets, norm_gain, proj_weight):
    rows, width = tokens.shape
    columns = proj_weight.shape[1]
    chunks = width // CHUNK
    col_tiles = columns // COLS
    half = rows // 2
    f32, bf16 = jnp.float32, jnp.bfloat16
    vmem, dma = pltpu.VMEM, pltpu.SemaphoreType.DMA
    piece = (K, CHUNK)
    return pl.pallas_call(
        functools.partial(kernel, seq_size),
        out_shape=jax.ShapeDtypeStruct((2 * K, columns), bf16),
        in_specs=[
            pl.BlockSpec(memory_space=pltpu.SMEM),
            pl.BlockSpec(memory_space=pltpu.VMEM),
            pl.BlockSpec(memory_space=pltpu.VMEM),
            pl.BlockSpec(memory_space=pl.ANY),
            pl.BlockSpec(memory_space=pl.ANY),
        ],
        out_specs=pl.BlockSpec(memory_space=pl.ANY),
        scratch_shapes=[
            vmem((chunks, 2, half, CHUNK), bf16),
            vmem((chunks, 2, CHUNK, half), bf16),
            vmem((col_tiles, width, COLS), bf16),
            vmem((col_tiles, 2 * K, COLS), bf16),
            vmem((2, 2 * K, half), f32),
            vmem((2, 2 * K, half), bf16),
            vmem((2, chunks, 2 * K, CHUNK), bf16),
            vmem((chunks, *piece), f32),
            vmem((chunks, *piece), f32),
            vmem((ROUNDS, chunks, *piece), f32),
            vmem((ROUNDS, chunks, *piece), f32),
            vmem((ROUNDS, chunks, *piece), bf16),
            vmem((ROUNDS, chunks, *piece), bf16),
            vmem((ITERS, chunks, *piece), bf16),
            vmem((ITERS, chunks, *piece), bf16),
            vmem((2, 2, K, 128), f32),
            vmem((K, 128), f32),
            vmem((K, 128), f32),
            vmem((ROUNDS, K, 128), f32),
            vmem((ROUNDS, K, 128), f32),
            vmem((ROUNDS, K, 128), f32),
            vmem((ROUNDS, K, 128), f32),
            vmem((2, K, 128), f32),
            vmem((chunks, *piece), f32),
            vmem((K, width), bf16),
            vmem((2 * K, width), bf16),
            dma((chunks, 2)),
            dma((col_tiles,)),
            dma((col_tiles,)),
            dma((ROUNDS, chunks)),
            dma((ROUNDS, chunks)),
            dma((ROUNDS, chunks)),
            dma((ROUNDS, chunks)),
            dma((ITERS, chunks)),
            dma((ITERS, chunks)),
            dma((ROUNDS,)),
            dma((ROUNDS,)),
            dma((ROUNDS,)),
            dma((ROUNDS,)),
            dma,
            dma,
        ],
        compiler_params=pltpu.CompilerParams(
            collective_id=0, has_side_effects=True, vmem_limit_bytes=60 * 2**20
        ),
    )(shot_starts, seed_offsets.T, norm_gain, tokens, proj_weight)


def solution(mesh):
    in_specs = (P(("seq", "feat"), None), P(), P(), P(), P(None, "feat"))
    out_specs = P("seq", "feat")
    return jax.shard_map(
        functools.partial(on_device, mesh.shape["seq"]),
        mesh=mesh,
        in_specs=in_specs,
        out_specs=out_specs,
        check_vma=False,
    )
```

```python
import functools
import math

import jax
import jax.numpy as jnp
from jax import lax
from jax.experimental import pallas as pl
from jax.experimental.pallas import tpu as pltpu
from jax.sharding import PartitionSpec as P

MESH = pl.DeviceIdType.MESH
ITERS = 3
ROUNDS = ITERS + 1
K = 64
CHUNK = 256
TILE = 256
COLS = 512
GROUPS = ((0, 1), (2, 3), (4,))


def kernel(
    seq_size,
    starts,
    seeds,
    gain,
    tok_hbm,
    w_hbm,
    out_hbm,
    x,
    xt,
    wp,
    outs,
    st,
    wt,
    c,
    po,
    px,
    si,
    qo,
    tb,
    ub,
    co,
    ci,
    mf,
    mx,
    mo,
    mi,
    mq,
    mt,
    mu,
    rec,
    cent,
    ns,
    nm,
    x_sem,
    w_sem,
    o_sem,
    p_send,
    p_recv,
    t_send,
    t_recv,
    c_send,
    c_recv,
    mp_send,
    mp_recv,
    mt_send,
    mt_recv,
    n_send,
    n_recv,
):
    chunks, _, half, _ = x.shape
    rows = 2 * half
    tiles = half // TILE
    col_tiles = wp.shape[0]
    width = chunks * CHUNK
    f32, bf16 = jnp.float32, jnp.bfloat16

    seq = lax.axis_index("seq")
    feat = lax.axis_index("feat")
    me = seq * 2 + feat
    count = seq_size * 2
    inner = (seq, 1 - feat)
    outer_seq = seq + 2 * feat - 1
    has_outer = jnp.logical_and(outer_seq >= 0, outer_seq < seq_size)
    outer = (outer_seq, 1 - feat)
    h_in, h_out = 1 - feat, feat

    def token_copy(f, h):
        return pltpu.make_async_copy(
            tok_hbm.at[
                pl.ds(pl.multiple_of(h * half, half), half),
                pl.ds(pl.multiple_of(f * CHUNK, CHUNK), CHUNK),
            ],
            x.at[f, h],
            x_sem.at[f, h],
        )

    def weight_copy(n):
        return pltpu.make_async_copy(
            w_hbm.at[:, pl.ds(pl.multiple_of(n * COLS, COLS), COLS)], wp.at[n], w_sem.at[n]
        )

    def out_copy(n):
        return pltpu.make_async_copy(
            outs.at[n], out_hbm.at[:, pl.ds(pl.multiple_of(n * COLS, COLS), COLS)], o_sem.at[n]
        )

    def remote(src, dst, send, recv, device):
        return pltpu.make_async_remote_copy(
            src_ref=src,
            dst_ref=dst,
            send_sem=send,
            recv_sem=recv,
            device_id=device,
            device_id_type=MESH,
        )

    def p_copy(r, g):
        at = pl.ds(GROUPS[g][0], len(GROUPS[g]))
        return remote(si.at[r, at], qo.at[r, at], p_send.at[r, g], p_recv.at[r, g], inner)

    def t_copy(r, g):
        at = pl.ds(GROUPS[g][0], len(GROUPS[g]))
        return remote(tb.at[r, at], ub.at[r, at], t_send.at[r, g], t_recv.at[r, g], outer)

    def c_copy(r, g):
        at = pl.ds(GROUPS[g][0], len(GROUPS[g]))
        return remote(co.at[r, at], ci.at[r, at], c_send.at[r, g], c_recv.at[r, g], inner)

    def mp_copy(r):
        return remote(mi.at[r], mq.at[r], mp_send.at[r], mp_recv.at[r], inner)

    def mt_copy(r):
        return remote(mt.at[r], mu.at[r], mt_send.at[r], mt_recv.at[r], outer)

    def n_copy():
        return remote(ns, nm.at[pl.ds(feat * K, K)], n_send, n_recv, inner)

    for f in range(chunks):
        token_copy(f, h_in).start()
    for f in range(chunks):
        token_copy(f, h_out).start()

    barrier = pltpu.get_barrier_semaphore()
    pl.semaphore_signal(barrier, inc=1, device_id=inner, device_id_type=MESH)

    @pl.when(has_outer)
    def _():
        pl.semaphore_signal(barrier, inc=1, device_id=outer, device_id_type=MESH)

    base = me * rows
    start = starts[me] - base
    after = jnp.minimum(me + 1, count - 1)
    end = jnp.where(me == count - 1, count * rows, starts[after]) - base

    def is_mine(shape):
        first = jnp.full(shape, start, jnp.int32) < 0
        last = jnp.full(shape, end, jnp.int32) >= rows
        left = jnp.full(shape, feat, jnp.int32) == 0
        return jnp.logical_or(
            jnp.logical_and(left, first), jnp.logical_and(jnp.logical_not(left), last)
        )

    @pl.when(jnp.logical_not(has_outer))
    def _():
        ub[...] = jnp.zeros_like(ub)
        mu[...] = jnp.zeros_like(mu)

    def column(shot, offset):
        shots = lax.broadcasted_iota(jnp.int32, seeds.shape, 1)
        picked = jnp.where(shots == shot, seeds[...], 0).astype(f32)
        return jnp.sum(picked, axis=1, keepdims=True).astype(jnp.int32) + offset

    own_at = column(me, start)
    next_at = column(after, end)

    def place(t):
        return slice(t * TILE, (t + 1) * TILE)

    def fold(w):
        total = w[:, :128]
        for i in range(1, TILE // 128):
            total = total + w[:, i * 128 : (i + 1) * 128]
        return total

    def put(h, t, nb, own):
        wt[h, :K, place(t)] = nb.astype(bf16)
        wt[h, K:, place(t)] = own.astype(bf16)

    def seed_weights(h):
        nb_mass, own_mass = 0.0, 0.0
        for t in range(tiles):
            at = lax.broadcasted_iota(jnp.int32, (K, TILE), 1) + (h * half + t * TILE)
            own = (at == own_at).astype(f32)
            nb = (at == next_at).astype(f32)
            put(h, t, nb, own)
            nb_mass, own_mass = nb_mass + fold(nb), own_mass + fold(own)
        mf[h, 0], mf[h, 1] = nb_mass, own_mass

    def group_score(group, h, at):
        total = 0.0
        for f in group:
            total = total + jnp.dot(c[h, f], xt[f, h, :, at], preferred_element_type=f32)
        return total

    def soften(h):
        scale = math.log2(math.e) / math.sqrt(width)
        nb_mass, own_mass = 0.0, 0.0
        for t in range(tiles):
            scores = st[h, :, place(t)] + group_score(GROUPS[-1], h, place(t))
            at = lax.broadcasted_iota(jnp.int32, (1, TILE), 1) + (h * half + t * TILE)
            is_nb = jnp.logical_or(at < start, at >= end)
            mixed = jnp.where(is_nb, scores[:K], scores[K:])
            e = jnp.exp2((mixed - jnp.max(mixed, axis=0, keepdims=True)) * scale)
            w = e * (1.0 / jnp.sum(e, axis=0, keepdims=True))
            nb = jnp.where(is_nb, w, 0.0)
            own = jnp.where(is_nb, 0.0, w)
            put(h, t, nb, own)
            nb_mass, own_mass = nb_mass + fold(nb), own_mass + fold(own)
        mf[h, 0], mf[h, 1] = nb_mass, own_mass

    def wide(m):
        return jnp.concatenate([m] * (CHUNK // 128), axis=1)

    def total_mass(m):
        return jnp.broadcast_to(jnp.sum(m, axis=1, keepdims=True), (K, 128))

    def sum_and_send(r, first):
        def partial(f, h):
            if first:
                token_copy(f, h).wait()
            return jnp.dot(wt[h], x[f, h], preferred_element_type=f32)

        for g, group in enumerate(GROUPS):
            for f in group:
                sums = partial(f, h_in)
                si[r, f] = sums[:K].astype(bf16)
                po[f] = sums[K:]
            if g == 0:
                mi[r] = total_mass(mf[h_in, 0])
                mp_copy(r).start()
            p_copy(r, g).start()
            if g == 0:
                mx[...] = total_mass(mf[h_out, 0])
                mo[...] = total_mass(mf[0, 1] + mf[1, 1])

        for g, group in enumerate(GROUPS):
            for f in group:
                sums = partial(f, h_out)
                px[f] = sums[:K]
                po[f] += sums[K:]
            if g == 0:
                mp_copy(r).wait_recv()
                chip = mo[...] + mq[r]
                mo[...] = chip
                mt[r] = jnp.where(is_mine((K, 128)), chip, mx[...])
            p_copy(r, g).wait_recv()
            for f in group:
                chip = po[f] + qo[r, f].astype(f32)
                po[f] = chip
                tb[r, f] = jnp.where(is_mine((K, CHUNK)), chip, px[f]).astype(bf16)

            @pl.when(has_outer)
            def _():
                if g == 0:
                    mt_copy(r).start()
                t_copy(r, g).start()

    def take_mass(r):
        @pl.when(has_outer)
        def _():
            mt_copy(r).wait_recv()

        mine = is_mine((K, 128))
        m_nb = mx[...] + jnp.where(mine, 0.0, mu[r])
        rec[0] = 1.0 / (mo[...] + jnp.where(mine, mu[r], 0.0))
        rec[1] = 1.0 / jnp.where(m_nb > 0.0, m_nb, 1.0)

    def arrive(r, g):
        @pl.when(has_outer)
        def _():
            t_copy(r, g).wait_recv()

    def own_total(r, f):
        return (
            po[f] + jnp.where(is_mine((K, CHUNK)), ub[r, f].astype(f32), 0.0)
        ) * wide(rec[0])

    def outer_total(r, f):
        return (
            px[f] + jnp.where(is_mine((K, CHUNK)), 0.0, ub[r, f].astype(f32))
        ) * wide(rec[1])

    def spread(r, g):
        arrive(r, g)
        for f in GROUPS[g]:
            own = own_total(r, f).astype(bf16)
            co[r, f] = own
            c[0, f, K:] = own
            c[1, f, K:] = own
        c_copy(r, g).start()
        for f in GROUPS[g]:
            c[h_out, f, :K] = outer_total(r, f).astype(bf16)

    def score(g, h):
        if g == len(GROUPS) - 1:
            soften(h)
            return
        for t in range(half // COLS):
            at = slice(t * COLS, (t + 1) * COLS)
            scores = group_score(GROUPS[g], h, at)
            if g:
                scores = scores + st[h, :, at]
            st[h, :, at] = scores

    def score_inner(r, g):
        c_copy(r, g).wait_recv()
        for f in GROUPS[g]:
            c[h_in, f, :K] = ci[r, f]
        score(g, h_in)

    seed_weights(h_in)
    seed_weights(h_out)
    pl.semaphore_wait(barrier, 1 + has_outer.astype(jnp.int32))
    sum_and_send(0, True)

    for n in range(col_tiles):
        weight_copy(n).start()

    @pl.loop(0, chunks)
    def _(f):
        for h in range(2):
            for t in range(tiles):
                xt[f, h, :, place(t)] = x[f, h, place(t)].T

    @pl.loop(0, ITERS)
    def _(r):
        take_mass(r)
        for g in range(len(GROUPS)):
            spread(r, g)
            score(g, h_out)
            if g:
                score_inner(r, g - 1)
        score_inner(r, len(GROUPS) - 1)
        sum_and_send(r + 1, False)

    take_mass(ITERS)
    square = jnp.zeros((K, 1), f32)
    for g, group in enumerate(GROUPS):
        arrive(ITERS, g)
        for f in group:
            own = own_total(ITERS, f)
            cent[f] = own
            square = square + jnp.sum(own * own, axis=1, keepdims=True)
    inverse = 1.0 / jnp.sqrt(square / width + 1e-06)
    for f in range(chunks):
        at = slice(f * CHUNK, (f + 1) * CHUNK)
        normed = (cent[f] * inverse * gain[at][None, :]).astype(bf16)
        ns[:, at] = normed
        nm[pl.ds(pl.multiple_of(feat * K, K), K), at] = normed
    n_copy().start()
    for n in range(col_tiles):
        weight_copy(n).wait()
    n_copy().wait_recv()

    for n in range(col_tiles):
        outs[n] = jnp.dot(nm[...], wp[n], preferred_element_type=f32).astype(bf16)
        if n % 2:
            out_copy(n - 1).start()
            out_copy(n).start()

    n_copy().wait_send()

    @pl.loop(0, ROUNDS)
    def _(r):
        mp_copy(r).wait_send()
        for g in range(len(GROUPS)):
            p_copy(r, g).wait_send()

        @pl.when(r < ITERS)
        def _():
            for g in range(len(GROUPS)):
                c_copy(r, g).wait_send()

        @pl.when(has_outer)
        def _():
            mt_copy(r).wait_send()
            for g in range(len(GROUPS)):
                t_copy(r, g).wait_send()

    for n in range(col_tiles):
        out_copy(n).wait()


def on_device(seq_size, tokens, shot_starts, seed_offsets, norm_gain, proj_weight):
    rows, width = tokens.shape
    columns = proj_weight.shape[1]
    chunks = width // CHUNK
    col_tiles = columns // COLS
    half = rows // 2
    f32, bf16 = jnp.float32, jnp.bfloat16
    vmem, dma = pltpu.VMEM, pltpu.SemaphoreType.DMA
    piece = (K, CHUNK)
    return pl.pallas_call(
        functools.partial(kernel, seq_size),
        out_shape=jax.ShapeDtypeStruct((2 * K, columns), bf16),
        in_specs=[
            pl.BlockSpec(memory_space=pltpu.SMEM),
            pl.BlockSpec(memory_space=pltpu.VMEM),
            pl.BlockSpec(memory_space=pltpu.VMEM),
            pl.BlockSpec(memory_space=pl.ANY),
            pl.BlockSpec(memory_space=pl.ANY),
        ],
        out_specs=pl.BlockSpec(memory_space=pl.ANY),
        scratch_shapes=[
            vmem((chunks, 2, half, CHUNK), bf16),
            vmem((chunks, 2, CHUNK, half), bf16),
            vmem((col_tiles, width, COLS), bf16),
            vmem((col_tiles, 2 * K, COLS), bf16),
            vmem((2, 2 * K, half), f32),
            vmem((2, 2 * K, half), bf16),
            vmem((2, chunks, 2 * K, CHUNK), bf16),
            vmem((chunks, *piece), f32),
            vmem((chunks, *piece), f32),
            vmem((ROUNDS, chunks, *piece), bf16),
            vmem((ROUNDS, chunks, *piece), bf16),
            vmem((ROUNDS, chunks, *piece), bf16),
            vmem((ROUNDS, chunks, *piece), bf16),
            vmem((ITERS, chunks, *piece), bf16),
            vmem((ITERS, chunks, *piece), bf16),
            vmem((2, 2, K, 128), f32),
            vmem((K, 128), f32),
            vmem((K, 128), f32),
            vmem((ROUNDS, K, 128), f32),
            vmem((ROUNDS, K, 128), f32),
            vmem((ROUNDS, K, 128), f32),
            vmem((ROUNDS, K, 128), f32),
            vmem((2, K, 128), f32),
            vmem((chunks, *piece), f32),
            vmem((K, width), bf16),
            vmem((2 * K, width), bf16),
            dma((chunks, 2)),
            dma((col_tiles,)),
            dma((col_tiles,)),
            dma((ROUNDS, len(GROUPS))),
            dma((ROUNDS, len(GROUPS))),
            dma((ROUNDS, len(GROUPS))),
            dma((ROUNDS, len(GROUPS))),
            dma((ITERS, len(GROUPS))),
            dma((ITERS, len(GROUPS))),
            dma((ROUNDS,)),
            dma((ROUNDS,)),
            dma((ROUNDS,)),
            dma((ROUNDS,)),
            dma,
            dma,
        ],
        compiler_params=pltpu.CompilerParams(
            collective_id=0, has_side_effects=True, vmem_limit_bytes=60 * 2**20
        ),
    )(shot_starts, seed_offsets.T, norm_gain, tokens, proj_weight)


def solution(mesh):
    in_specs = (P(("seq", "feat"), None), P(), P(), P(), P(None, "feat"))
    out_specs = P("seq", "feat")
    return jax.shard_map(
        functools.partial(on_device, mesh.shape["seq"]),
        mesh=mesh,
        in_specs=in_specs,
        out_specs=out_specs,
        check_vma=False,
    )
```

```python
import functools
import math

import jax
import jax.numpy as jnp
from jax import lax
from jax.experimental import pallas as pl
from jax.experimental.pallas import tpu as pltpu
from jax.sharding import PartitionSpec as P

MESH = pl.DeviceIdType.MESH
ITERS = 3
ROUNDS = ITERS + 1
K = 64
CHUNK = 256
TILE = 256
COLS = 512
GROUPS = ((0, 1), (2, 3, 4))


def kernel(
    seq_size,
    starts,
    seeds,
    gain,
    tok_hbm,
    w_hbm,
    nm,
    wp,
    x,
    xt,
    st,
    wt,
    c,
    po,
    px,
    si,
    qo,
    tb,
    ub,
    co,
    ci,
    mf,
    mx,
    mo,
    mi,
    mq,
    mt,
    mu,
    rec,
    cent,
    ns,
    nr,
    x_sem,
    w_sem,
    p_send,
    p_recv,
    t_send,
    t_recv,
    c_send,
    c_recv,
    mp_send,
    mp_recv,
    mt_send,
    mt_recv,
    n_send,
    n_recv,
):
    chunks, _, half, _ = x.shape
    rows = 2 * half
    tiles = half // TILE
    col_tiles = wp.shape[0]
    width = chunks * CHUNK
    f32, bf16 = jnp.float32, jnp.bfloat16

    seq = lax.axis_index("seq")
    feat = lax.axis_index("feat")
    me = seq * 2 + feat
    count = seq_size * 2
    inner = (seq, 1 - feat)
    outer_seq = seq + 2 * feat - 1
    has_outer = jnp.logical_and(outer_seq >= 0, outer_seq < seq_size)
    outer = (outer_seq, 1 - feat)
    h_in, h_out = 1 - feat, feat

    def token_copy(f, h):
        return pltpu.make_async_copy(
            tok_hbm.at[
                pl.ds(pl.multiple_of(h * half, half), half),
                pl.ds(pl.multiple_of(f * CHUNK, CHUNK), CHUNK),
            ],
            x.at[f, h],
            x_sem.at[f, h],
        )

    def weight_copy(n):
        return pltpu.make_async_copy(
            w_hbm.at[:, pl.ds(pl.multiple_of(n * COLS, COLS), COLS)], wp.at[n], w_sem.at[n]
        )

    def remote(src, dst, send, recv, device):
        return pltpu.make_async_remote_copy(
            src_ref=src,
            dst_ref=dst,
            send_sem=send,
            recv_sem=recv,
            device_id=device,
            device_id_type=MESH,
        )

    def p_copy(r, g):
        at = pl.ds(GROUPS[g][0], len(GROUPS[g]))
        return remote(si.at[r, at], qo.at[r, at], p_send.at[r, g], p_recv.at[r, g], inner)

    def t_copy(r, g):
        at = pl.ds(GROUPS[g][0], len(GROUPS[g]))
        return remote(tb.at[r, at], ub.at[r, at], t_send.at[r, g], t_recv.at[r, g], outer)

    def c_copy(r, g):
        at = pl.ds(GROUPS[g][0], len(GROUPS[g]))
        return remote(co.at[r, at], ci.at[r, at], c_send.at[r, g], c_recv.at[r, g], inner)

    def mp_copy(r):
        return remote(mi.at[r], mq.at[r], mp_send.at[r], mp_recv.at[r], inner)

    def mt_copy(r):
        return remote(mt.at[r], mu.at[r], mt_send.at[r], mt_recv.at[r], outer)

    def n_copy():
        return remote(ns, nr, n_send, n_recv, inner)

    for f in range(chunks):
        token_copy(f, h_in).start()
    for f in range(chunks):
        token_copy(f, h_out).start()

    barrier = pltpu.get_barrier_semaphore()
    pl.semaphore_signal(barrier, inc=1, device_id=inner, device_id_type=MESH)

    @pl.when(has_outer)
    def _():
        pl.semaphore_signal(barrier, inc=1, device_id=outer, device_id_type=MESH)

    base = me * rows
    start = starts[me] - base
    after = jnp.minimum(me + 1, count - 1)
    end = jnp.where(me == count - 1, count * rows, starts[after]) - base

    def is_mine(shape):
        first = jnp.full(shape, start, jnp.int32) < 0
        last = jnp.full(shape, end, jnp.int32) >= rows
        left = jnp.full(shape, feat, jnp.int32) == 0
        return jnp.logical_or(
            jnp.logical_and(left, first), jnp.logical_and(jnp.logical_not(left), last)
        )

    @pl.when(jnp.logical_not(has_outer))
    def _():
        ub[...] = jnp.zeros_like(ub)
        mu[...] = jnp.zeros_like(mu)

    def column(shot, offset):
        shots = lax.broadcasted_iota(jnp.int32, seeds.shape, 1)
        picked = jnp.where(shots == shot, seeds[...], 0).astype(f32)
        return jnp.sum(picked, axis=1, keepdims=True).astype(jnp.int32) + offset

    own_at = column(me, start)
    next_at = column(after, end)

    def place(t):
        return slice(t * TILE, (t + 1) * TILE)

    def fold(w):
        total = w[:, :128]
        for i in range(1, TILE // 128):
            total = total + w[:, i * 128 : (i + 1) * 128]
        return total

    def put(h, t, nb, own):
        wt[h, :K, place(t)] = nb.astype(bf16)
        wt[h, K:, place(t)] = own.astype(bf16)

    def seed_weights(h):
        nb_mass, own_mass = 0.0, 0.0
        for t in range(tiles):
            at = lax.broadcasted_iota(jnp.int32, (K, TILE), 1) + (h * half + t * TILE)
            own = (at == own_at).astype(f32)
            nb = (at == next_at).astype(f32)
            put(h, t, nb, own)
            nb_mass, own_mass = nb_mass + fold(nb), own_mass + fold(own)
        mf[h, 0], mf[h, 1] = nb_mass, own_mass

    def group_score(group, h, at):
        total = 0.0
        for f in group:
            total = total + jnp.dot(c[h, f], xt[f, h, :, at], preferred_element_type=f32)
        return total

    def soften(h):
        scale = math.log2(math.e) / math.sqrt(width)
        nb_mass, own_mass = 0.0, 0.0
        for t in range(tiles):
            scores = st[h, :, place(t)] + group_score(GROUPS[-1], h, place(t))
            at = lax.broadcasted_iota(jnp.int32, (1, TILE), 1) + (h * half + t * TILE)
            is_nb = jnp.logical_or(at < start, at >= end)
            mixed = jnp.where(is_nb, scores[:K], scores[K:])
            e = jnp.exp2((mixed - jnp.max(mixed, axis=0, keepdims=True)) * scale)
            w = e * (1.0 / jnp.sum(e, axis=0, keepdims=True))
            nb = jnp.where(is_nb, w, 0.0)
            own = jnp.where(is_nb, 0.0, w)
            put(h, t, nb, own)
            nb_mass, own_mass = nb_mass + fold(nb), own_mass + fold(own)
        mf[h, 0], mf[h, 1] = nb_mass, own_mass

    def wide(m):
        return jnp.concatenate([m] * (CHUNK // 128), axis=1)

    def total_mass(m):
        return jnp.broadcast_to(jnp.sum(m, axis=1, keepdims=True), (K, 128))

    def sum_and_send(r, first):
        def partial(f, h):
            if first:
                token_copy(f, h).wait()
            return jnp.dot(wt[h], x[f, h], preferred_element_type=f32)

        for g, group in enumerate(GROUPS):
            for f in group:
                sums = partial(f, h_in)
                si[r, f] = sums[:K].astype(bf16)
                po[f] = sums[K:]
            if g == 0:
                mi[r] = total_mass(mf[h_in, 0])
                mp_copy(r).start()
            p_copy(r, g).start()
            if g == 0:
                mx[...] = total_mass(mf[h_out, 0])
                mo[...] = total_mass(mf[0, 1] + mf[1, 1])

        for g, group in enumerate(GROUPS):
            for f in group:
                sums = partial(f, h_out)
                px[f] = sums[:K]
                po[f] += sums[K:]
            if g == 0:
                mp_copy(r).wait_recv()
                chip = mo[...] + mq[r]
                mo[...] = chip
                mt[r] = jnp.where(is_mine((K, 128)), chip, mx[...])
            p_copy(r, g).wait_recv()
            for f in group:
                chip = po[f] + qo[r, f].astype(f32)
                po[f] = chip
                tb[r, f] = jnp.where(is_mine((K, CHUNK)), chip, px[f]).astype(bf16)

            @pl.when(has_outer)
            def _():
                if g == 0:
                    mt_copy(r).start()
                t_copy(r, g).start()

    def take_mass(r):
        @pl.when(has_outer)
        def _():
            mt_copy(r).wait_recv()

        mine = is_mine((K, 128))
        m_nb = mx[...] + jnp.where(mine, 0.0, mu[r])
        rec[0] = 1.0 / (mo[...] + jnp.where(mine, mu[r], 0.0))
        rec[1] = 1.0 / jnp.where(m_nb > 0.0, m_nb, 1.0)

    def arrive(r, g):
        @pl.when(has_outer)
        def _():
            t_copy(r, g).wait_recv()

    def own_total(r, f):
        return (
            po[f] + jnp.where(is_mine((K, CHUNK)), ub[r, f].astype(f32), 0.0)
        ) * wide(rec[0])

    def outer_total(r, f):
        return (
            px[f] + jnp.where(is_mine((K, CHUNK)), 0.0, ub[r, f].astype(f32))
        ) * wide(rec[1])

    def spread(r, g):
        arrive(r, g)
        for f in GROUPS[g]:
            own = own_total(r, f).astype(bf16)
            co[r, f] = own
            c[0, f, K:] = own
            c[1, f, K:] = own
        c_copy(r, g).start()
        for f in GROUPS[g]:
            c[h_out, f, :K] = outer_total(r, f).astype(bf16)

    def score(g, h):
        if g == len(GROUPS) - 1:
            soften(h)
            return
        for t in range(half // COLS):
            at = slice(t * COLS, (t + 1) * COLS)
            scores = group_score(GROUPS[g], h, at)
            if g:
                scores = scores + st[h, :, at]
            st[h, :, at] = scores

    def score_inner(r, g):
        c_copy(r, g).wait_recv()
        for f in GROUPS[g]:
            c[h_in, f, :K] = ci[r, f]
        score(g, h_in)

    seed_weights(h_in)
    seed_weights(h_out)
    pl.semaphore_wait(barrier, 1 + has_outer.astype(jnp.int32))
    sum_and_send(0, True)

    for n in range(col_tiles):
        weight_copy(n).start()

    @pl.loop(0, chunks)
    def _(f):
        for h in range(2):
            for t in range(tiles):
                xt[f, h, :, place(t)] = x[f, h, place(t)].T

    @pl.loop(0, ITERS)
    def _(r):
        take_mass(r)
        for g in range(len(GROUPS)):
            spread(r, g)
            score(g, h_out)
            if g:
                score_inner(r, g - 1)
        score_inner(r, len(GROUPS) - 1)
        sum_and_send(r + 1, False)

    take_mass(ITERS)
    square = jnp.zeros((K, 1), f32)
    for g, group in enumerate(GROUPS):
        arrive(ITERS, g)
        for f in group:
            own = own_total(ITERS, f)
            cent[f] = own
            square = square + jnp.sum(own * own, axis=1, keepdims=True)
    inverse = 1.0 / jnp.sqrt(square / width + 1e-06)
    for f in range(chunks):
        at = slice(f * CHUNK, (f + 1) * CHUNK)
        normed = (cent[f] * inverse * gain[at][None, :]).astype(bf16)
        ns[:, at] = normed
        nm[pl.ds(pl.multiple_of(feat * K, K), K), at] = normed
    n_copy().start()
    for n in range(col_tiles):
        weight_copy(n).wait()
    n_copy().wait_recv()
    nm[pl.ds(pl.multiple_of((1 - feat) * K, K), K)] = nr[...]

    n_copy().wait_send()

    @pl.loop(0, ROUNDS)
    def _(r):
        mp_copy(r).wait_send()
        for g in range(len(GROUPS)):
            p_copy(r, g).wait_send()

        @pl.when(r < ITERS)
        def _():
            for g in range(len(GROUPS)):
                c_copy(r, g).wait_send()

        @pl.when(has_outer)
        def _():
            mt_copy(r).wait_send()
            for g in range(len(GROUPS)):
                t_copy(r, g).wait_send()


def project(nm, wp, out_hbm, outs, o_sem):
    def out_copy(n):
        return pltpu.make_async_copy(
            outs.at[n], out_hbm.at[:, pl.ds(n * COLS, COLS)], o_sem.at[n]
        )

    col_tiles = wp.shape[0]
    for n in range(col_tiles):
        outs[n] = jnp.dot(nm[...], wp[n], preferred_element_type=jnp.float32).astype(jnp.bfloat16)
        if n % 2:
            out_copy(n - 1).start()
            out_copy(n).start()
    for n in range(col_tiles):
        out_copy(n).wait()


def on_device(seq_size, tokens, shot_starts, seed_offsets, norm_gain, proj_weight):
    rows, width = tokens.shape
    columns = proj_weight.shape[1]
    chunks = width // CHUNK
    col_tiles = columns // COLS
    half = rows // 2
    f32, bf16 = jnp.float32, jnp.bfloat16
    vmem, dma = pltpu.VMEM, pltpu.SemaphoreType.DMA
    piece = (K, CHUNK)
    normed, weights = pl.pallas_call(
        functools.partial(kernel, seq_size),
        out_shape=(vmem((2 * K, width), bf16), vmem((col_tiles, width, COLS), bf16)),
        in_specs=[
            pl.BlockSpec(memory_space=pltpu.SMEM),
            pl.BlockSpec(memory_space=pltpu.VMEM),
            pl.BlockSpec(memory_space=pltpu.VMEM),
            pl.BlockSpec(memory_space=pl.ANY),
            pl.BlockSpec(memory_space=pl.ANY),
        ],
        out_specs=(pl.BlockSpec(memory_space=pltpu.VMEM),) * 2,
        scratch_shapes=[
            vmem((chunks, 2, half, CHUNK), bf16),
            vmem((chunks, 2, CHUNK, half), bf16),
            vmem((2, 2 * K, half), f32),
            vmem((2, 2 * K, half), bf16),
            vmem((2, chunks, 2 * K, CHUNK), bf16),
            vmem((chunks, *piece), f32),
            vmem((chunks, *piece), f32),
            vmem((ROUNDS, chunks, *piece), bf16),
            vmem((ROUNDS, chunks, *piece), bf16),
            vmem((ROUNDS, chunks, *piece), bf16),
            vmem((ROUNDS, chunks, *piece), bf16),
            vmem((ITERS, chunks, *piece), bf16),
            vmem((ITERS, chunks, *piece), bf16),
            vmem((2, 2, K, 128), f32),
            vmem((K, 128), f32),
            vmem((K, 128), f32),
            vmem((ROUNDS, K, 128), f32),
            vmem((ROUNDS, K, 128), f32),
            vmem((ROUNDS, K, 128), f32),
            vmem((ROUNDS, K, 128), f32),
            vmem((2, K, 128), f32),
            vmem((chunks, *piece), f32),
            vmem((K, width), bf16),
            vmem((K, width), bf16),
            dma((chunks, 2)),
            dma((col_tiles,)),
            dma((ROUNDS, len(GROUPS))),
            dma((ROUNDS, len(GROUPS))),
            dma((ROUNDS, len(GROUPS))),
            dma((ROUNDS, len(GROUPS))),
            dma((ITERS, len(GROUPS))),
            dma((ITERS, len(GROUPS))),
            dma((ROUNDS,)),
            dma((ROUNDS,)),
            dma((ROUNDS,)),
            dma((ROUNDS,)),
            dma,
            dma,
        ],
        compiler_params=pltpu.CompilerParams(
            collective_id=0, has_side_effects=True, vmem_limit_bytes=46 * 2**20
        ),
    )(shot_starts, seed_offsets.T, norm_gain, tokens, proj_weight)
    return pl.pallas_call(
        project,
        out_shape=jax.ShapeDtypeStruct((2 * K, columns), bf16),
        in_specs=[pl.BlockSpec(memory_space=pltpu.VMEM)] * 2,
        out_specs=pl.BlockSpec(memory_space=pl.ANY),
        scratch_shapes=[vmem((col_tiles, 2 * K, COLS), bf16), dma((col_tiles,))],
        compiler_params=pltpu.CompilerParams(vmem_limit_bytes=20 * 2**20),
    )(normed, weights)


def solution(mesh):
    in_specs = (P(("seq", "feat"), None), P(), P(), P(), P(None, "feat"))
    out_specs = P("seq", "feat")
    return jax.shard_map(
        functools.partial(on_device, mesh.shape["seq"]),
        mesh=mesh,
        in_specs=in_specs,
        out_specs=out_specs,
        check_vma=False,
    )
```

```python
import functools
import math

import jax
import jax.numpy as jnp
from jax import lax
from jax.experimental import pallas as pl
from jax.experimental.pallas import tpu as pltpu
from jax.sharding import PartitionSpec as P

MESH = pl.DeviceIdType.MESH
ITERS = 3
ROUNDS = ITERS + 1
K = 64
CHUNK = 256
TILE = 256
COLS = 512
GROUPS = ((0,), (1, 2), (3, 4))


def kernel(
    seq_size,
    starts,
    seeds,
    gain,
    tok_hbm,
    w_hbm,
    nm,
    wp,
    x,
    xt,
    st,
    wt,
    c,
    po,
    px,
    si,
    qo,
    tb,
    ub,
    co,
    ci,
    mf,
    mx,
    mo,
    mi,
    mq,
    mt,
    mu,
    rec,
    cent,
    ns,
    nr,
    x_sem,
    w_sem,
    p_send,
    p_recv,
    t_send,
    t_recv,
    c_send,
    c_recv,
    mp_send,
    mp_recv,
    mt_send,
    mt_recv,
    n_send,
    n_recv,
):
    chunks, _, half, _ = x.shape
    rows = 2 * half
    tiles = half // TILE
    col_tiles = wp.shape[0]
    width = chunks * CHUNK
    f32, bf16 = jnp.float32, jnp.bfloat16

    seq = lax.axis_index("seq")
    feat = lax.axis_index("feat")
    me = seq * 2 + feat
    count = seq_size * 2
    inner = (seq, 1 - feat)
    outer_seq = seq + 2 * feat - 1
    has_outer = jnp.logical_and(outer_seq >= 0, outer_seq < seq_size)
    outer = (outer_seq, 1 - feat)
    h_in, h_out = 1 - feat, feat

    def token_copy(f, h):
        return pltpu.make_async_copy(
            tok_hbm.at[
                pl.ds(pl.multiple_of(h * half, half), half),
                pl.ds(pl.multiple_of(f * CHUNK, CHUNK), CHUNK),
            ],
            x.at[f, h],
            x_sem.at[f, h],
        )

    def weight_copy(n):
        return pltpu.make_async_copy(
            w_hbm.at[:, pl.ds(pl.multiple_of(n * COLS, COLS), COLS)], wp.at[n], w_sem.at[n]
        )

    def remote(src, dst, send, recv, device):
        return pltpu.make_async_remote_copy(
            src_ref=src,
            dst_ref=dst,
            send_sem=send,
            recv_sem=recv,
            device_id=device,
            device_id_type=MESH,
        )

    def p_copy(r, g):
        at = pl.ds(GROUPS[g][0], len(GROUPS[g]))
        return remote(si.at[r, at], qo.at[r, at], p_send.at[r, g], p_recv.at[r, g], inner)

    def t_copy(r, g):
        at = pl.ds(GROUPS[g][0], len(GROUPS[g]))
        return remote(tb.at[r, at], ub.at[r, at], t_send.at[r, g], t_recv.at[r, g], outer)

    def c_copy(r, g):
        at = pl.ds(GROUPS[g][0], len(GROUPS[g]))
        return remote(co.at[r, at], ci.at[r, at], c_send.at[r, g], c_recv.at[r, g], inner)

    def mp_copy(r):
        return remote(mi.at[r], mq.at[r], mp_send.at[r], mp_recv.at[r], inner)

    def mt_copy(r):
        return remote(mt.at[r], mu.at[r], mt_send.at[r], mt_recv.at[r], outer)

    def n_copy():
        return remote(ns, nr, n_send, n_recv, inner)

    for f in range(chunks):
        token_copy(f, h_in).start()
    for f in range(chunks):
        token_copy(f, h_out).start()

    barrier = pltpu.get_barrier_semaphore()
    pl.semaphore_signal(barrier, inc=1, device_id=inner, device_id_type=MESH)

    @pl.when(has_outer)
    def _():
        pl.semaphore_signal(barrier, inc=1, device_id=outer, device_id_type=MESH)

    base = me * rows
    start = starts[me] - base
    after = jnp.minimum(me + 1, count - 1)
    end = jnp.where(me == count - 1, count * rows, starts[after]) - base

    def is_mine(shape):
        first = jnp.full(shape, start, jnp.int32) < 0
        last = jnp.full(shape, end, jnp.int32) >= rows
        left = jnp.full(shape, feat, jnp.int32) == 0
        return jnp.logical_or(
            jnp.logical_and(left, first), jnp.logical_and(jnp.logical_not(left), last)
        )

    @pl.when(jnp.logical_not(has_outer))
    def _():
        ub[...] = jnp.zeros_like(ub)
        mu[...] = jnp.zeros_like(mu)

    def column(shot, offset):
        shots = lax.broadcasted_iota(jnp.int32, seeds.shape, 1)
        picked = jnp.where(shots == shot, seeds[...], 0).astype(f32)
        return jnp.sum(picked, axis=1, keepdims=True).astype(jnp.int32) + offset

    own_at = column(me, start)
    next_at = column(after, end)

    def place(t):
        return slice(t * TILE, (t + 1) * TILE)

    def fold(w):
        total = w[:, :128]
        for i in range(1, TILE // 128):
            total = total + w[:, i * 128 : (i + 1) * 128]
        return total

    def put(h, t, nb, own):
        wt[h, :K, place(t)] = nb.astype(bf16)
        wt[h, K:, place(t)] = own.astype(bf16)

    def seed_weights(h):
        nb_mass, own_mass = 0.0, 0.0
        for t in range(tiles):
            at = lax.broadcasted_iota(jnp.int32, (K, TILE), 1) + (h * half + t * TILE)
            own = (at == own_at).astype(f32)
            nb = (at == next_at).astype(f32)
            put(h, t, nb, own)
            nb_mass, own_mass = nb_mass + fold(nb), own_mass + fold(own)
        mf[h, 0], mf[h, 1] = nb_mass, own_mass

    def group_score(group, h, at):
        total = 0.0
        for f in group:
            total = total + jnp.dot(c[h, f], xt[f, h, :, at], preferred_element_type=f32)
        return total

    def soften(h):
        scale = math.log2(math.e) / math.sqrt(width)
        nb_mass, own_mass = 0.0, 0.0
        for t in range(tiles):
            scores = st[h, :, place(t)] + group_score(GROUPS[-1], h, place(t))
            at = lax.broadcasted_iota(jnp.int32, (1, TILE), 1) + (h * half + t * TILE)
            is_nb = jnp.logical_or(at < start, at >= end)
            mixed = jnp.where(is_nb, scores[:K], scores[K:])
            e = jnp.exp2((mixed - jnp.max(mixed, axis=0, keepdims=True)) * scale)
            share = 1.0 / jnp.sum(e, axis=0, keepdims=True)
            nb = e * jnp.where(is_nb, share, 0.0)
            own = e * jnp.where(is_nb, 0.0, share)
            put(h, t, nb, own)
            nb_mass, own_mass = nb_mass + fold(nb), own_mass + fold(own)
        mf[h, 0], mf[h, 1] = nb_mass, own_mass

    def wide(m):
        return jnp.concatenate([m] * (CHUNK // 128), axis=1)

    def total_mass(m):
        return jnp.broadcast_to(jnp.sum(m, axis=1, keepdims=True), (K, 128))

    def partial(f, h, first=False):
        if first:
            token_copy(f, h).wait()
        return jnp.dot(wt[h], x[f, h], preferred_element_type=f32)

    def sum_early():
        for f in GROUPS[0]:
            sums = partial(f, h_out)
            px[f] = sums[:K]
            po[f] = sums[K:]

    def sum_and_send(r, first):
        for g, group in enumerate(GROUPS):
            for f in group:
                sums = partial(f, h_in, first)
                si[r, f] = sums[:K].astype(bf16)
                po[f] = sums[K:] if g or first else po[f] + sums[K:]
            if first and g == 0:
                pl.semaphore_wait(barrier, 1 + has_outer.astype(jnp.int32))
            if g == 0:
                mi[r] = total_mass(mf[h_in, 0])
                mp_copy(r).start()
            p_copy(r, g).start()
            if g == 0:
                mx[...] = total_mass(mf[h_out, 0])
                mo[...] = total_mass(mf[0, 1] + mf[1, 1])

        for g, group in enumerate(GROUPS):
            for f in group if g or first else ():
                sums = partial(f, h_out, first)
                px[f] = sums[:K]
                po[f] += sums[K:]
            if g == 0:
                mp_copy(r).wait_recv()
                chip = mo[...] + mq[r]
                mo[...] = chip
                mt[r] = jnp.where(is_mine((K, 128)), chip, mx[...])
            p_copy(r, g).wait_recv()
            for f in group:
                chip = po[f] + qo[r, f].astype(f32)
                po[f] = chip
                tb[r, f] = jnp.where(is_mine((K, CHUNK)), chip, px[f]).astype(bf16)

            @pl.when(has_outer)
            def _():
                if g == 0:
                    mt_copy(r).start()
                t_copy(r, g).start()

    def take_mass(r):
        @pl.when(has_outer)
        def _():
            mt_copy(r).wait_recv()

        mine = is_mine((K, 128))
        m_nb = mx[...] + jnp.where(mine, 0.0, mu[r])
        rec[0] = 1.0 / (mo[...] + jnp.where(mine, mu[r], 0.0))
        rec[1] = 1.0 / jnp.where(m_nb > 0.0, m_nb, 1.0)

    def arrive(r, g):
        @pl.when(has_outer)
        def _():
            t_copy(r, g).wait_recv()

    def own_total(r, f):
        return (
            po[f] + jnp.where(is_mine((K, CHUNK)), ub[r, f].astype(f32), 0.0)
        ) * wide(rec[0])

    def outer_total(r, f):
        return (
            px[f] + jnp.where(is_mine((K, CHUNK)), 0.0, ub[r, f].astype(f32))
        ) * wide(rec[1])

    def spread(r, g):
        arrive(r, g)
        for f in GROUPS[g]:
            own = own_total(r, f).astype(bf16)
            co[r, f] = own
            c[0, f, K:] = own
            c[1, f, K:] = own
        c_copy(r, g).start()
        for f in GROUPS[g]:
            c[h_out, f, :K] = outer_total(r, f).astype(bf16)

    def score(g, h):
        if g == len(GROUPS) - 1:
            soften(h)
            return
        for t in range(half // COLS):
            at = slice(t * COLS, (t + 1) * COLS)
            scores = group_score(GROUPS[g], h, at)
            if g:
                scores = scores + st[h, :, at]
            st[h, :, at] = scores

    def score_inner(r, g):
        c_copy(r, g).wait_recv()
        for f in GROUPS[g]:
            c[h_in, f, :K] = ci[r, f]
        score(g, h_in)

    seed_weights(h_in)
    seed_weights(h_out)
    sum_and_send(0, True)

    for n in range(col_tiles):
        weight_copy(n).start()

    @pl.loop(0, chunks)
    def _(f):
        for h in range(2):
            for t in range(tiles):
                xt[f, h, :, place(t)] = x[f, h, place(t)].T

    @pl.loop(0, ITERS)
    def _(r):
        take_mass(r)
        for g in range(len(GROUPS)):
            spread(r, g)
            score(g, h_out)
            if g:
                score_inner(r, g - 1)
        sum_early()
        score_inner(r, len(GROUPS) - 1)
        sum_and_send(r + 1, False)

    take_mass(ITERS)
    square = jnp.zeros((K, 1), f32)
    for g, group in enumerate(GROUPS):
        arrive(ITERS, g)
        for f in group:
            own = own_total(ITERS, f)
            cent[f] = own
            square = square + jnp.sum(own * own, axis=1, keepdims=True)
    inverse = 1.0 / jnp.sqrt(square / width + 1e-06)
    for f in range(chunks):
        at = slice(f * CHUNK, (f + 1) * CHUNK)
        normed = (cent[f] * inverse * gain[at][None, :]).astype(bf16)
        ns[:, at] = normed
        nm[pl.ds(pl.multiple_of(feat * K, K), K), at] = normed
    n_copy().start()
    for n in range(col_tiles):
        weight_copy(n).wait()
    n_copy().wait_recv()
    nm[pl.ds(pl.multiple_of((1 - feat) * K, K), K)] = nr[...]

    n_copy().wait_send()

    @pl.loop(0, ROUNDS)
    def _(r):
        mp_copy(r).wait_send()
        for g in range(len(GROUPS)):
            p_copy(r, g).wait_send()

        @pl.when(r < ITERS)
        def _():
            for g in range(len(GROUPS)):
                c_copy(r, g).wait_send()

        @pl.when(has_outer)
        def _():
            mt_copy(r).wait_send()
            for g in range(len(GROUPS)):
                t_copy(r, g).wait_send()


def project(nm, wp, out_hbm, outs, o_sem):
    def out_copy(n):
        return pltpu.make_async_copy(
            outs.at[n], out_hbm.at[:, pl.ds(n * COLS, COLS)], o_sem.at[n]
        )

    col_tiles = wp.shape[0]
    for n in range(col_tiles):
        outs[n] = jnp.dot(nm[...], wp[n], preferred_element_type=jnp.float32).astype(jnp.bfloat16)
        if n % 2:
            out_copy(n - 1).start()
            out_copy(n).start()
    for n in range(col_tiles):
        out_copy(n).wait()


def on_device(seq_size, tokens, shot_starts, seed_offsets, norm_gain, proj_weight):
    rows, width = tokens.shape
    columns = proj_weight.shape[1]
    chunks = width // CHUNK
    col_tiles = columns // COLS
    half = rows // 2
    f32, bf16 = jnp.float32, jnp.bfloat16
    vmem, dma = pltpu.VMEM, pltpu.SemaphoreType.DMA
    piece = (K, CHUNK)
    normed, weights = pl.pallas_call(
        functools.partial(kernel, seq_size),
        out_shape=(vmem((2 * K, width), bf16), vmem((col_tiles, width, COLS), bf16)),
        in_specs=[
            pl.BlockSpec(memory_space=pltpu.SMEM),
            pl.BlockSpec(memory_space=pltpu.VMEM),
            pl.BlockSpec(memory_space=pltpu.VMEM),
            pl.BlockSpec(memory_space=pl.ANY),
            pl.BlockSpec(memory_space=pl.ANY),
        ],
        out_specs=(pl.BlockSpec(memory_space=pltpu.VMEM),) * 2,
        scratch_shapes=[
            vmem((chunks, 2, half, CHUNK), bf16),
            vmem((chunks, 2, CHUNK, half), bf16),
            vmem((2, 2 * K, half), f32),
            vmem((2, 2 * K, half), bf16),
            vmem((2, chunks, 2 * K, CHUNK), bf16),
            vmem((chunks, *piece), f32),
            vmem((chunks, *piece), f32),
            vmem((ROUNDS, chunks, *piece), bf16),
            vmem((ROUNDS, chunks, *piece), bf16),
            vmem((ROUNDS, chunks, *piece), bf16),
            vmem((ROUNDS, chunks, *piece), bf16),
            vmem((ITERS, chunks, *piece), bf16),
            vmem((ITERS, chunks, *piece), bf16),
            vmem((2, 2, K, 128), f32),
            vmem((K, 128), f32),
            vmem((K, 128), f32),
            vmem((ROUNDS, K, 128), f32),
            vmem((ROUNDS, K, 128), f32),
            vmem((ROUNDS, K, 128), f32),
            vmem((ROUNDS, K, 128), f32),
            vmem((2, K, 128), f32),
            vmem((chunks, *piece), f32),
            vmem((K, width), bf16),
            vmem((K, width), bf16),
            dma((chunks, 2)),
            dma((col_tiles,)),
            dma((ROUNDS, len(GROUPS))),
            dma((ROUNDS, len(GROUPS))),
            dma((ROUNDS, len(GROUPS))),
            dma((ROUNDS, len(GROUPS))),
            dma((ITERS, len(GROUPS))),
            dma((ITERS, len(GROUPS))),
            dma((ROUNDS,)),
            dma((ROUNDS,)),
            dma((ROUNDS,)),
            dma((ROUNDS,)),
            dma,
            dma,
        ],
        compiler_params=pltpu.CompilerParams(
            collective_id=0, has_side_effects=True, vmem_limit_bytes=46 * 2**20
        ),
    )(shot_starts, seed_offsets.T, norm_gain, tokens, proj_weight)
    return pl.pallas_call(
        project,
        out_shape=jax.ShapeDtypeStruct((2 * K, columns), bf16),
        in_specs=[pl.BlockSpec(memory_space=pltpu.VMEM)] * 2,
        out_specs=pl.BlockSpec(memory_space=pl.ANY),
        scratch_shapes=[vmem((col_tiles, 2 * K, COLS), bf16), dma((col_tiles,))],
        compiler_params=pltpu.CompilerParams(vmem_limit_bytes=20 * 2**20),
    )(normed, weights)


def solution(mesh):
    in_specs = (P(("seq", "feat"), None), P(), P(), P(), P(None, "feat"))
    out_specs = P("seq", "feat")
    return jax.shard_map(
        functools.partial(on_device, mesh.shape["seq"]),
        mesh=mesh,
        in_specs=in_specs,
        out_specs=out_specs,
        check_vma=False,
    )
```
